32 devices in a mesh: gz: 8 (over z, y), gy: 4 (over x, core).
Axes of the slice: x: 2, y: 2, z: 4, core: 2. Of those that a mesh axis runs over, the one named last changes fastest.
Arguments:
- charge: float32 [393216], P(('gz', 'gy')), may hold values from -4 to 4
- fractions: float32 [3, 393216], P(None, ('gz', 'gy')), may hold values from 0 to 1
- cell_base: int32 [3, 393216], P(None, ('gz', 'gy')), may hold values from 0 to 255, as said below
- live_blocks: int32 [8, 4], P('gz'), may hold values from 12 to 96, as said below
- send_blocks: int32 [8, 4], P('gz'), may hold values from 0 to 36, as said below
- moduli: float32 [3, 256], replicated, may hold values from 0.5 to 2
- screening: float32 [1], replicated, may hold values from 8 to 16
Outputs:
- forces: float32 [3, 393216], P(None, ('gz', 'gy'))
The draws below stay inside these ranges and needn't reach their ends.
Inputs may be any that keep to these rules, and one draw needn't show every extreme that they name: `cell_base`: row 0 lies in 0 to 31, row 1 in 0 to 63, row 2 in 0 to 255. `live_blocks`: a domain's live blocks are its first ones; in every row of the table some domain has 96 live blocks. send_blocks is at most the domain's live blocks; live_blocks minus send_blocks plus send_blocks of the domain before it along gy (cyclically) is at most 96; in every row some domain sends 36.
All inputs are finite; a program needn't handle non-finite values.
Results may differ from the reference program's by a relative error of at most 0.00023.
Values sent between devices are 32-bit elements; how exact they have to be, the bound alone decides.
A program may use at most 128 MiB of HBM per device.

```python
import math
import jax
import jax.numpy as jnp

GRID = 256
BLOCK = 128
NBLK = 96
ATOMS_DEV = 12288
ATOMS = 393216
PZ = 32
PY = 64
SEND_MAX = 36
LOW = 12
N_GZ = 8
N_GY = 4


def migration_plan(key):
    base_key = jax.random.fold_in(key, 7)
    key_load, key_busy = jax.random.split(base_key)
    drawn = jax.random.randint(key_load, (N_GZ, N_GY), 0, 1001)
    powered = drawn * drawn // 1000
    powered = powered * powered // 1000
    live_count = LOW + (NBLK - LOW) * powered // 1000
    busiest = jax.random.randint(key_busy, (N_GZ, 1), 0, N_GY)
    lane_ids = jnp.arange(N_GY, dtype=jnp.int32)[None, :]
    live_count = jnp.where(lane_ids == busiest, NBLK, live_count)
    live_count = jnp.where(lane_ids == jnp.mod(busiest + 1, N_GY), LOW, live_count)
    following = jnp.roll(live_count, -1, axis=1)
    send_count = jnp.clip((live_count - following + 1) // 2, 0, SEND_MAX)
    return (live_count.astype(jnp.int32), send_count.astype(jnp.int32))


def draw_live_blocks(key, part):
    return migration_plan(key)[0]


def draw_send_blocks(key, part):
    return migration_plan(key)[1]


def draw_cell_base(key, part):
    key_z, key_y, key_x = jax.random.split(jax.random.fold_in(key, 11), 3)
    rows_z = jax.random.randint(key_z, (ATOMS,), 0, PZ)
    rows_y = jax.random.randint(key_y, (ATOMS,), 0, PY)
    rows_x = jax.random.randint(key_x, (ATOMS,), 0, GRID)
    return jnp.stack([rows_z, rows_y, rows_x]).astype(jnp.int32)


def steps_of(key, extent, cuts, low, high):
    def one(axis_at, shards_of):
        draws = jax.random.uniform(jax.random.fold_in(jax.random.fold_in(key, 6), axis_at), (shards_of,), jnp.float32, low / len(cuts), high / len(cuts))
        return jnp.repeat(jnp.exp(draws), extent[axis_at] // shards_of).reshape((-1,) + (1,) * (len(extent) - axis_at - 1))

    level = one(*cuts[0])
    for cut in cuts[1:]:
        level = level * one(*cut)
    return level


def normal_values(stream_key, shape, scale, limit, shards=(), held_as=jnp.bfloat16):
    factor_of = steps_of(stream_key, shape, shards, -0.22, 0.18) if shards else 1.0
    array = jax.random.normal(stream_key, shape, jnp.float32) * scale * factor_of
    return jnp.minimum(jnp.maximum(array, -limit), limit).astype(held_as)


def setup_inputs(seed: int = 0) -> dict:
    splits = jax.random.split(jax.random.key(seed), 8)
    charge = normal_values(splits[0], (ATOMS,), 1.0, 4.0, ((0, 32),), jnp.float32)
    fractions = jnp.clip(1.0 * jax.random.uniform(splits[1], (3, ATOMS), jnp.float32) ** steps_of(splits[1], (3, ATOMS), ((1, 32),), -0.2, 0.2), 0.0, 1.0)
    cell_base = draw_cell_base(jax.random.fold_in(splits[7], 71), 0)
    live_blocks = draw_live_blocks(jax.random.fold_in(splits[7], 71), 0)
    send_blocks = draw_send_blocks(jax.random.fold_in(splits[7], 71), 0)
    moduli = jnp.clip(jnp.exp(jax.random.uniform(splits[5], (3, GRID), jnp.float32, math.log(0.5), math.log(2.0))), 0.5, 2.0)
    screening = jnp.clip(jnp.exp(jax.random.uniform(splits[6], (1,), jnp.float32, math.log(8.0), math.log(16.0))), 8.0, 16.0)
    return {"charge": charge, "fractions": fractions, "cell_base": cell_base, "live_blocks": live_blocks, "send_blocks": send_blocks, "moduli": moduli, "screening": screening}


coulomb = 2.0


def spline_weights(fractions_row):
    remain = 1.0 - fractions_row
    square = fractions_row * fractions_row
    cubed = square * fractions_row
    weights = [remain * remain * remain / 6.0,
               (3.0 * cubed - 6.0 * square + 4.0) / 6.0,
               (-3.0 * cubed + 3.0 * square + 3.0 * fractions_row + 1.0) / 6.0,
               cubed / 6.0]
    slopes = [-0.5 * remain * remain,
              1.5 * square - 2.0 * fractions_row,
              -1.5 * square + fractions_row + 0.5,
              0.5 * square]
    return weights, slopes


def reference(charge, fractions, cell_base, live_blocks, send_blocks, moduli, screening):
    atom_index = jnp.arange(ATOMS, dtype=jnp.int32)
    device_index = atom_index // ATOMS_DEV
    slab_index = device_index // N_GY
    column_index = device_index % N_GY
    slot_index = atom_index % ATOMS_DEV
    live_count = live_blocks[slab_index, column_index]
    weighted = jnp.where(slot_index // BLOCK < live_count, charge, 0.0)
    weight_z, slope_z = spline_weights(fractions[0])
    weight_y, slope_y = spline_weights(fractions[1])
    weight_x, slope_x = spline_weights(fractions[2])
    base_z = slab_index * PZ + cell_base[0]
    base_y = column_index * PY + cell_base[1]
    base_x = cell_base[2]
    density = jnp.zeros((GRID * GRID * GRID,), jnp.float32)
    for shift_z in range(4):
        index_z = jnp.mod(base_z + shift_z, GRID)
        for shift_y in range(4):
            index_y = jnp.mod(base_y + shift_y, GRID)
            for shift_x in range(4):
                index_x = jnp.mod(base_x + shift_x, GRID)
                flat_index = ((index_z * GRID + index_y) * GRID + index_x).astype(jnp.int32)
                density = density.at[flat_index].add(weighted * weight_z[shift_z] * weight_y[shift_y] * weight_x[shift_x])
    density = density.reshape(GRID, GRID, GRID)
    spectrum = jnp.fft.fftn(density)
    waves = jnp.arange(GRID, dtype=jnp.int32)
    signed_wave = jnp.where(waves < GRID // 2, waves, waves - GRID)
    wave_square = signed_wave * signed_wave
    radius = wave_square[:, None, None] + wave_square[None, :, None] + wave_square[None, None, :]
    squared = radius.astype(jnp.float32) / float(GRID * GRID)
    product = coulomb * moduli[0][:, None, None] * moduli[1][None, :, None] * moduli[2][None, None, :]
    safe_squared = jnp.where(radius > 0, squared, 1.0)
    kernel = jnp.where(radius > 0, product * jnp.exp(-screening[0] * squared) / safe_squared, 0.0)
    potential = jnp.real(jnp.fft.ifftn(spectrum * kernel)).astype(jnp.float32)
    flat_potential = potential.reshape(-1)
    force_z = jnp.zeros((ATOMS,), jnp.float32)
    force_y = jnp.zeros((ATOMS,), jnp.float32)
    force_x = jnp.zeros((ATOMS,), jnp.float32)
    for shift_z in range(4):
        index_z = jnp.mod(base_z + shift_z, GRID)
        for shift_y in range(4):
            index_y = jnp.mod(base_y + shift_y, GRID)
            for shift_x in range(4):
                index_x = jnp.mod(base_x + shift_x, GRID)
                flat_index = ((index_z * GRID + index_y) * GRID + index_x).astype(jnp.int32)
                values = flat_potential[flat_index]
                force_z = force_z + slope_z[shift_z] * weight_y[shift_y] * weight_x[shift_x] * values
                force_y = force_y + weight_z[shift_z] * slope_y[shift_y] * weight_x[shift_x] * values
                force_x = force_x + weight_z[shift_z] * weight_y[shift_y] * slope_x[shift_x] * values
    home = -weighted[None, :] * jnp.stack([force_z, force_y, force_x])
    domains = N_GZ * N_GY
    home = home.reshape(3, domains, ATOMS_DEV)
    live_flat = live_blocks.reshape(-1)
    send_flat = send_blocks.reshape(-1)
    devices = jnp.arange(domains, dtype=jnp.int32)
    column_of = devices % N_GY
    previous = (devices - column_of + jnp.mod(column_of - 1, N_GY)).astype(jnp.int32)
    kept_atoms = (live_flat - send_flat) * BLOCK
    arriving = send_flat[previous] * BLOCK
    source_start = (live_flat[previous] - send_flat[previous]) * BLOCK
    slots = jnp.arange(ATOMS_DEV, dtype=jnp.int32)
    own_forces = jnp.where(slots[None, None, :] < kept_atoms[None, :, None], home, 0.0)
    guest_slot = slots[None, :] - kept_atoms[:, None] + source_start[:, None]
    valid = (slots[None, :] >= kept_atoms[:, None]) & (slots[None, :] < kept_atoms[:, None] + arriving[:, None])
    guest_slot = jnp.clip(guest_slot, 0, ATOMS_DEV - 1).astype(jnp.int32)
    neighbour = home[:, previous, :]
    guest = jnp.take_along_axis(neighbour, guest_slot[None, :, :], axis=2)
    result = own_forces + jnp.where(valid[None, :, :], guest, 0.0)
    return result.reshape(3, ATOMS)
```

```python
import functools

import jax
import jax.numpy as jnp
import numpy as np
from jax import lax
from jax.experimental import pallas as pl
from jax.experimental.pallas import tpu as pltpu
from jax.sharding import PartitionSpec as P

BLOCK = 128
SEND_MAX = 36
GROUP = 256
CHUNK = 4

high = lax.Precision.HIGH
coulomb = 2.0


def shifted(x, axis, by):
    peers = lax.axis_size(axis)
    return lax.ppermute(x, axis, [(i, (i + by) % peers) for i in range(peers)])


def round_up(value, step):
    return -(-value // step) * step


def spline_weights(t):
    remain = 1.0 - t
    square = t * t
    cubed = square * t
    weights = [
        remain * remain * remain * (1.0 / 6.0),
        (3.0 * cubed - 6.0 * square + 4.0) * (1.0 / 6.0),
        (-3.0 * cubed + 3.0 * square + 3.0 * t + 1.0) * (1.0 / 6.0),
        cubed * (1.0 / 6.0),
    ]
    slopes = [
        -0.5 * remain * remain,
        1.5 * square - 2.0 * t,
        -1.5 * square + t + 0.5,
        0.5 * square,
    ]
    return weights, slopes


def stencil(base, weights, span, wrap):
    offset = lax.broadcasted_iota(jnp.int32, (span, base.shape[1]), 0) - base
    if wrap:
        offset = jnp.where(offset < 0, offset + span, offset)
    table = jnp.where(offset == 0, weights[0], 0.0)
    for k in range(1, 4):
        table = jnp.where(offset == k, weights[k], table)
    return table


def split(value):
    top = value.astype(jnp.bfloat16)
    rest = (value - top.astype(jnp.float32)).astype(jnp.bfloat16)
    return top, rest


def spread_kernel(planes, rows, grid, count, floats, cells, tile, table_z, factor_x):
    tile[...] = jnp.zeros_like(tile)
    atoms = count[0]

    @pl.loop(0, (atoms + GROUP - 1) // GROUP)
    def _(group):
        at = pl.ds(pl.multiple_of(group * GROUP, GROUP), GROUP)
        place = group * GROUP + lax.broadcasted_iota(jnp.int32, (1, GROUP), 1)
        charge = jnp.where(place < atoms, floats[0:1, at], 0.0)
        weight_z, _ = spline_weights(floats[1:2, at])
        weight_y, _ = spline_weights(floats[2:3, at])
        weight_x, _ = spline_weights(floats[3:4, at])
        weight_x = [charge * w for w in weight_x]
        table_z[...] = stencil(cells[0:1, at], weight_z, planes, False)
        table_y = stencil(cells[1:2, at], weight_y, rows, False)
        top, rest = split(stencil(cells[2:3, at], weight_x, grid, True))
        factor_x[:, :GROUP] = top
        factor_x[:, GROUP : 2 * GROUP] = top
        factor_x[:, 2 * GROUP :] = rest

        @pl.loop(0, planes // CHUNK)
        def _(chunk):
            part = jnp.concatenate(
                [table_z[pl.ds(chunk * CHUNK + j, 1), :] * table_y for j in range(CHUNK)], 0
            )
            top, rest = split(part)
            where = pl.ds(pl.multiple_of(chunk * (CHUNK * rows), CHUNK * rows), CHUNK * rows)
            tile[where, :] += lax.dot_general(
                jnp.concatenate([top, rest, top], 1),
                factor_x[...],
                (((1,), (1,)), ((), ())),
                preferred_element_type=jnp.float32,
            )


def interpolate_kernel(
    planes, rows, grid, count, floats, cells, tile, forces,
    factor_tile, factor_x, table_z, rising_z, sum_w, sum_g, sum_x,
):
    forces[...] = jnp.zeros_like(forces)
    atoms = count[0]
    span = CHUNK * rows

    @pl.loop(0, planes // CHUNK)
    def _(chunk):
        where = pl.ds(pl.multiple_of(chunk * span, span), span)
        top, rest = split(tile[where, :])
        factor_tile[where, :grid] = top
        factor_tile[where, grid : 2 * grid] = rest
        factor_tile[where, 2 * grid :] = top

    @pl.loop(0, (atoms + GROUP - 1) // GROUP)
    def _(group):
        at = pl.ds(pl.multiple_of(group * GROUP, GROUP), GROUP)
        place = group * GROUP + lax.broadcasted_iota(jnp.int32, (1, GROUP), 1)
        charge = -jnp.where(place < atoms, floats[0:1, at], 0.0)
        weight_z, slope_z = spline_weights(floats[1:2, at])
        weight_x, slope_x = spline_weights(floats[3:4, at])
        table_z[...] = stencil(cells[0:1, at], weight_z, planes, False)
        rising_z[...] = stencil(cells[0:1, at], slope_z, planes, False)
        for half, values in enumerate((weight_x, slope_x)):
            top, rest = split(stencil(cells[2:3, at], values, grid, True))
            columns = slice(half * GROUP, (half + 1) * GROUP)
            factor_x[:grid, columns] = top
            factor_x[grid : 2 * grid, columns] = top
            factor_x[2 * grid :, columns] = rest
        sum_w[...] = jnp.zeros_like(sum_w)
        sum_g[...] = jnp.zeros_like(sum_g)
        sum_x[...] = jnp.zeros_like(sum_x)

        @pl.loop(0, planes // CHUNK)
        def _(chunk):
            where = pl.ds(pl.multiple_of(chunk * span, span), span)
            along = jnp.dot(
                factor_tile[where, :], factor_x[...], preferred_element_type=jnp.float32
            )
            zs = [table_z[pl.ds(chunk * CHUNK + j, 1), :] for j in range(CHUNK)]
            gs = [rising_z[pl.ds(chunk * CHUNK + j, 1), :] for j in range(CHUNK)]
            for r in range(0, rows, 8):
                local = slice(r, r + 8)
                w = [along[j * rows + r : j * rows + r + 8, :GROUP] for j in range(CHUNK)]
                s = [along[j * rows + r : j * rows + r + 8, GROUP:] for j in range(CHUNK)]
                sum_w[local, :] += sum(zs[j] * w[j] for j in range(CHUNK))
                sum_g[local, :] += sum(gs[j] * w[j] for j in range(CHUNK))
                sum_x[local, :] += sum(zs[j] * s[j] for j in range(CHUNK))

        weight_y, slope_y = spline_weights(floats[2:3, at])
        table_y = stencil(cells[1:2, at], weight_y, rows, False)
        rising_y = stencil(cells[1:2, at], slope_y, rows, False)
        forces[0:1, at] = charge * jnp.sum(table_y * sum_g[...], 0, keepdims=True)
        forces[1:2, at] = charge * jnp.sum(rising_y * sum_w[...], 0, keepdims=True)
        forces[2:3, at] = charge * jnp.sum(table_y * sum_x[...], 0, keepdims=True)


def vmem():
    return pl.BlockSpec(memory_space=pltpu.VMEM)


def smem():
    return pl.BlockSpec(memory_space=pltpu.SMEM)


def spread_atoms(count, floats, cells, planes, rows, grid):
    return pl.pallas_call(
        functools.partial(spread_kernel, planes, rows, grid),
        out_shape=jax.ShapeDtypeStruct((planes * rows, grid), jnp.float32),
        in_specs=[smem(), vmem(), vmem()],
        out_specs=vmem(),
        scratch_shapes=[
            pltpu.VMEM((planes, GROUP), jnp.float32),
            pltpu.VMEM((grid, 3 * GROUP), jnp.bfloat16),
        ],
        cost_estimate=pl.CostEstimate(
            flops=planes * rows * grid * floats.shape[1] * 4,
            bytes_accessed=planes * rows * grid * 4,
            transcendentals=0,
        ),
        name="spread",
    )(count, floats, cells)


def interpolate_atoms(count, floats, cells, tile, planes, rows, grid):
    return pl.pallas_call(
        functools.partial(interpolate_kernel, planes, rows, grid),
        out_shape=jax.ShapeDtypeStruct((3, floats.shape[1]), jnp.float32),
        in_specs=[smem(), vmem(), vmem(), vmem()],
        out_specs=vmem(),
        scratch_shapes=[
            pltpu.VMEM((planes * rows, 3 * grid), jnp.bfloat16),
            pltpu.VMEM((3 * grid, 2 * GROUP), jnp.bfloat16),
            pltpu.VMEM((planes, GROUP), jnp.float32),
            pltpu.VMEM((planes, GROUP), jnp.float32),
            pltpu.VMEM((rows, GROUP), jnp.float32),
            pltpu.VMEM((rows, GROUP), jnp.float32),
            pltpu.VMEM((rows, GROUP), jnp.float32),
        ],
        cost_estimate=pl.CostEstimate(
            flops=planes * rows * grid * floats.shape[1] * 8,
            bytes_accessed=planes * rows * grid * 4,
            transcendentals=0,
        ),
        name="interpolate",
    )(count, floats, cells, tile)


def turns(grid, wave, place, quarter):
    whole = np.mod(wave * place + (grid // 4) * quarter, grid)
    return np.cos(2.0 * np.pi * whole / grid).astype(np.float32)


def wave_tables(grid, slabs, columns, waves):
    kx = np.arange(slabs * waves).reshape(slabs, 1, waves)
    part = np.arange(2)
    x = np.arange(grid)
    table_x = turns(grid, kx[None], x[:, None, None, None], part[None, None, :, None])
    kz = np.arange(grid).reshape(columns, 1, grid // columns, 1, 1)
    table_z = turns(
        grid, kz, x[None, None, None, :, None],
        part[None, :, None, None, None] - part[None, None, None, None, :],
    ).reshape(2 * grid, 2 * grid)
    y = np.arange(grid).reshape(columns, 1, grid // columns, 1, 1)
    table_y = turns(
        grid, x[None, None, None, None, :], y,
        part[None, None, None, :, None] - part[None, :, None, None, None],
    )
    return table_x, table_z, table_y


def signed_wave(waves, grid):
    return jnp.where(waves < grid // 2, waves, waves - grid)


def influence(moduli, screening, slab, column, grid, count_kx, count_kz):
    kx = slab * count_kx + lax.iota(jnp.int32, count_kx)
    kz = column * count_kz + lax.iota(jnp.int32, count_kz)
    ky = lax.iota(jnp.int32, grid)
    half = grid // 2
    share = jnp.where((kx == 0) | (kx == half), 1.0, 2.0)
    share = jnp.where(kx <= half, share, 0.0) * (0.5 * coulomb / grid**3)
    nx, nz, ny = (signed_wave(k, grid) for k in (kx, kz, ky))
    radius = (nz * nz)[:, None, None] + (nx * nx)[None, :, None] + (ny * ny)[None, None, :]
    squared = radius.astype(jnp.float32) / float(grid * grid)
    mirrored = jnp.roll(moduli[:, ::-1], 1, 1)
    spare = jnp.zeros((count_kx * lax.axis_size("gz"),), jnp.float32)

    def product(table):
        mx = lax.dynamic_slice_in_dim(
            jnp.concatenate([table[2], spare]), slab * count_kx, count_kx, 0
        )
        mz = lax.dynamic_slice_in_dim(table[0], column * count_kz, count_kz, 0)
        return mz[:, None, None] * (share * mx)[None, :, None] * table[1][None, None, :]

    both = product(moduli) + product(mirrored)
    safe = jnp.where(radius > 0, squared, 1.0)
    return jnp.where(radius > 0, both * jnp.exp(-screening[0] * squared) / safe, 0.0)


def exchange(x, axis):
    return lax.all_to_all(x, axis, split_axis=0, concat_axis=0, tiled=True)


def contract(form, *operands):
    return jnp.einsum(form, *operands, precision=high, preferred_element_type=jnp.float32)


def potential_field(block, kernel, tables, slabs, columns, waves):
    table_x, table_z, table_y = tables
    planes, rows, grid = block.shape
    lanes = waves * rows
    spectrum = contract("zyx,xpck->pzcky", block, table_x)
    spectrum = exchange(spectrum.reshape(slabs * planes * 2, lanes), "gz")
    spectrum = contract("mn,nl->ml", table_z, spectrum)
    spectrum = exchange(spectrum, "gy").reshape(columns, 2, grid // columns, waves, rows)
    spectrum = contract("pczky,pcydw->zkdw", spectrum, table_y)
    spectrum = spectrum * kernel[:, :, None, :]
    spectrum = contract("zkdw,pcydw->pczky", spectrum, table_y)
    spectrum = exchange(spectrum.reshape(2 * grid, lanes), "gy")
    spectrum = contract("mn,ml->nl", table_z, spectrum)
    spectrum = exchange(spectrum, "gz").reshape(slabs, planes, 2, waves, rows)
    return contract("pzcky,xpck->zyx", spectrum, table_x)


def solve_tile(volume, kernel, tables, planes, rows, waves, slabs, columns):
    span_planes, span_rows, grid = volume.shape
    rim_planes = shifted(volume[planes : planes + 3], "gz", 1)
    volume = jnp.concatenate([volume[:3] + rim_planes, volume[3:planes]], 0)
    rim_rows = shifted(volume[:, rows : rows + 3], "gy", 1)
    block = jnp.concatenate([volume[:, :3] + rim_rows, volume[:, 3:rows]], 1)
    potential = potential_field(block, kernel, tables, slabs, columns, waves)
    upper_rows = shifted(potential[:, :3], "gy", -1)
    spare_rows = jnp.zeros((planes, span_rows - rows - 3, grid), jnp.float32)
    widened = jnp.concatenate([potential, upper_rows, spare_rows], 1)
    upper_planes = shifted(widened[:3], "gz", -1)
    spare_planes = jnp.zeros((span_planes - planes - 3, span_rows, grid), jnp.float32)
    return jnp.concatenate([widened, upper_planes, spare_planes], 0)


def body(charge, fractions, cell_base, live_blocks, send_blocks, moduli, screening):
    slabs = lax.axis_size("gz")
    columns = lax.axis_size("gy")
    grid = moduli.shape[1]
    planes = grid // slabs
    rows = grid // columns
    span_planes = round_up(planes + 3, CHUNK)
    span_rows = round_up(rows + 3, 8)
    waves = -(-(grid // 2 + 1) // slabs)
    slab = lax.axis_index("gz")
    column = lax.axis_index("gy")
    lane_ids = lax.iota(jnp.int32, columns)
    live = jnp.sum(jnp.where(lane_ids == column, live_blocks[0], 0))
    send = jnp.sum(jnp.where(lane_ids == column, send_blocks[0], 0))
    before = jnp.sum(
        jnp.where(lane_ids == jnp.mod(column - 1, columns), send_blocks[0], 0)
    )
    kept_atoms = (live - send) * BLOCK
    moved_count = (before * BLOCK)[None]
    margin = SEND_MAX * BLOCK
    own_floats = jnp.concatenate([charge[None, :], fractions], 0)
    float_rows = jnp.concatenate([own_floats, jnp.zeros((4, margin), jnp.float32)], 1)
    cell_rows = jnp.concatenate([cell_base, jnp.zeros((3, margin), jnp.int32)], 1)
    lent_floats = lax.dynamic_slice_in_dim(float_rows, kept_atoms, margin, 1)
    lent_cells = lax.dynamic_slice_in_dim(cell_rows, kept_atoms, margin, 1)
    moved = shifted(lent_floats, "gy", 1)
    moved_cells = shifted(lent_cells, "gy", 1)
    sizes = (span_planes, span_rows, grid)
    tables = wave_tables(grid, slabs, columns, waves)
    kernel = influence(moduli, screening, slab, column, grid, waves, grid // columns)
    foreign = spread_atoms(moved_count, moved, moved_cells, *sizes)
    own_count, foreign, kernel = lax.optimization_barrier((kept_atoms[None], foreign, kernel))
    returned = shifted(foreign, "gy", -1)
    own = spread_atoms(own_count, own_floats, cell_base, *sizes)
    padded = solve_tile(
        (own + returned).reshape(sizes), kernel, tables, planes, rows, waves, slabs, columns
    ).reshape(span_planes * span_rows, grid)
    borrowed = shifted(padded, "gy", 1)
    own_forces = interpolate_atoms(own_count, own_floats, cell_base, padded, *sizes)
    own_forces, borrowed = lax.optimization_barrier((own_forces, borrowed))
    arrivals = interpolate_atoms(moved_count, moved, moved_cells, borrowed, *sizes)
    holder = jnp.zeros((3, charge.shape[0] + margin), jnp.float32)
    holder = lax.dynamic_update_slice(holder, arrivals, (jnp.zeros((), jnp.int32), kept_atoms))
    return own_forces + holder[:, : charge.shape[0]]


def solution(mesh):
    return jax.shard_map(
        body,
        mesh=mesh,
        in_specs=(
            P(("gz", "gy")),
            P(None, ("gz", "gy")),
            P(None, ("gz", "gy")),
            P("gz", None),
            P("gz", None),
            P(),
            P(),
        ),
        out_specs=P(None, ("gz", "gy")),
        check_vma=False,
    )
```

```python
import functools

import jax
import jax.numpy as jnp
import numpy as np
from jax import lax
from jax.experimental import pallas as pl
from jax.experimental.pallas import tpu as pltpu
from jax.sharding import PartitionSpec as P

BLOCK = 128
SEND_MAX = 36
GROUP = 256

high = lax.Precision.HIGH
coulomb = 2.0


def shifted(x, axis, by):
    peers = lax.axis_size(axis)
    return lax.ppermute(x, axis, [(i, (i + by) % peers) for i in range(peers)])


def round_up(value, step):
    return -(-value // step) * step


def spline_weights(t):
    remain = 1.0 - t
    square = t * t
    cubed = square * t
    weights = [
        remain * remain * remain * (1.0 / 6.0),
        (3.0 * cubed - 6.0 * square + 4.0) * (1.0 / 6.0),
        (-3.0 * cubed + 3.0 * square + 3.0 * t + 1.0) * (1.0 / 6.0),
        cubed * (1.0 / 6.0),
    ]
    slopes = [
        -0.5 * remain * remain,
        1.5 * square - 2.0 * t,
        -1.5 * square + t + 0.5,
        0.5 * square,
    ]
    return weights, slopes


def stencil(base, weights, span, wrap):
    offset = lax.broadcasted_iota(jnp.int32, (span, base.shape[1]), 0) - base
    if wrap:
        offset = jnp.where(offset < 0, offset + span, offset)
    table = jnp.where(offset == 0, weights[0], 0.0)
    for k in range(1, 4):
        table = jnp.where(offset == k, weights[k], table)
    return table


def split(value):
    top = value.astype(jnp.bfloat16)
    rest = (value - top.astype(jnp.float32)).astype(jnp.bfloat16)
    return top, rest


def spread_kernel(planes, rows, grid, count, floats, cells, tile, table_z, factor_x):
    tile[...] = jnp.zeros_like(tile)
    atoms = count[0]

    @pl.loop(0, (atoms + GROUP - 1) // GROUP)
    def _(group):
        at = pl.ds(pl.multiple_of(group * GROUP, GROUP), GROUP)
        place = group * GROUP + lax.broadcasted_iota(jnp.int32, (1, GROUP), 1)
        charge = jnp.where(place < atoms, floats[0:1, at], 0.0)
        weight_z, _ = spline_weights(floats[1:2, at])
        weight_y, _ = spline_weights(floats[2:3, at])
        weight_x, _ = spline_weights(floats[3:4, at])
        weight_x = [charge * w for w in weight_x]
        table_z[...] = stencil(cells[0:1, at], weight_z, planes, False)
        table_y = stencil(cells[1:2, at], weight_y, rows, False)
        top, rest = split(stencil(cells[2:3, at], weight_x, grid, True))
        factor_x[:, :GROUP] = top
        factor_x[:, GROUP : 2 * GROUP] = top
        factor_x[:, 2 * GROUP :] = rest

        part = jnp.concatenate([table_z[j : j + 1, :] * table_y for j in range(planes)], 0)
        top, rest = split(part)
        tile[...] += lax.dot_general(
            jnp.concatenate([top, rest, top], 1),
            factor_x[...],
            (((1,), (1,)), ((), ())),
            preferred_element_type=jnp.float32,
        )


def interpolate_kernel(
    planes, rows, grid, count, floats, cells, tile, forces,
    factor_tile, factor_x, table_z, rising_z, sum_w, sum_g, sum_x,
):
    forces[...] = jnp.zeros_like(forces)
    atoms = count[0]

    @pl.loop(0, planes // 2)
    def _(chunk):
        where = pl.ds(pl.multiple_of(chunk * (2 * rows), 2 * rows), 2 * rows)
        top, rest = split(tile[where, :])
        factor_tile[where, :grid] = top
        factor_tile[where, grid : 2 * grid] = rest
        factor_tile[where, 2 * grid :] = top

    @pl.loop(0, (atoms + GROUP - 1) // GROUP)
    def _(group):
        at = pl.ds(pl.multiple_of(group * GROUP, GROUP), GROUP)
        place = group * GROUP + lax.broadcasted_iota(jnp.int32, (1, GROUP), 1)
        charge = -jnp.where(place < atoms, floats[0:1, at], 0.0)
        weight_z, slope_z = spline_weights(floats[1:2, at])
        weight_x, slope_x = spline_weights(floats[3:4, at])
        table_z[...] = stencil(cells[0:1, at], weight_z, planes, False)
        rising_z[...] = stencil(cells[0:1, at], slope_z, planes, False)
        for half, values in enumerate((weight_x, slope_x)):
            top, rest = split(stencil(cells[2:3, at], values, grid, True))
            columns = slice(half * GROUP, (half + 1) * GROUP)
            factor_x[:grid, columns] = top
            factor_x[grid : 2 * grid, columns] = top
            factor_x[2 * grid :, columns] = rest
        along = jnp.dot(factor_tile[...], factor_x[...], preferred_element_type=jnp.float32)
        zs = [table_z[j : j + 1, :] for j in range(planes)]
        gs = [rising_z[j : j + 1, :] for j in range(planes)]
        for r in range(0, rows, 8):
            local = slice(r, r + 8)
            w = [along[j * rows + r : j * rows + r + 8, :GROUP] for j in range(planes)]
            s = [along[j * rows + r : j * rows + r + 8, GROUP:] for j in range(planes)]
            sum_w[local, :] = sum(zs[j] * w[j] for j in range(planes))
            sum_g[local, :] = sum(gs[j] * w[j] for j in range(planes))
            sum_x[local, :] = sum(zs[j] * s[j] for j in range(planes))

        weight_y, slope_y = spline_weights(floats[2:3, at])
        table_y = stencil(cells[1:2, at], weight_y, rows, False)
        rising_y = stencil(cells[1:2, at], slope_y, rows, False)
        forces[0:1, at] = charge * jnp.sum(table_y * sum_g[...], 0, keepdims=True)
        forces[1:2, at] = charge * jnp.sum(rising_y * sum_w[...], 0, keepdims=True)
        forces[2:3, at] = charge * jnp.sum(table_y * sum_x[...], 0, keepdims=True)


def vmem():
    return pl.BlockSpec(memory_space=pltpu.VMEM)


def smem():
    return pl.BlockSpec(memory_space=pltpu.SMEM)


def spread_atoms(count, floats, cells, planes, rows, grid):
    return pl.pallas_call(
        functools.partial(spread_kernel, planes, rows, grid),
        out_shape=jax.ShapeDtypeStruct((planes * rows, grid), jnp.float32),
        in_specs=[smem(), vmem(), vmem()],
        out_specs=vmem(),
        scratch_shapes=[
            pltpu.VMEM((planes, GROUP), jnp.float32),
            pltpu.VMEM((grid, 3 * GROUP), jnp.bfloat16),
        ],
        cost_estimate=pl.CostEstimate(
            flops=planes * rows * grid * floats.shape[1] * 4,
            bytes_accessed=planes * rows * grid * 4,
            transcendentals=0,
        ),
        name="spread",
    )(count, floats, cells)


def interpolate_atoms(count, floats, cells, tile, planes, rows, grid):
    return pl.pallas_call(
        functools.partial(interpolate_kernel, planes, rows, grid),
        out_shape=jax.ShapeDtypeStruct((3, floats.shape[1]), jnp.float32),
        in_specs=[smem(), vmem(), vmem(), vmem()],
        out_specs=vmem(),
        scratch_shapes=[
            pltpu.VMEM((planes * rows, 3 * grid), jnp.bfloat16),
            pltpu.VMEM((3 * grid, 2 * GROUP), jnp.bfloat16),
            pltpu.VMEM((planes, GROUP), jnp.float32),
            pltpu.VMEM((planes, GROUP), jnp.float32),
            pltpu.VMEM((rows, GROUP), jnp.float32),
            pltpu.VMEM((rows, GROUP), jnp.float32),
            pltpu.VMEM((rows, GROUP), jnp.float32),
        ],
        cost_estimate=pl.CostEstimate(
            flops=planes * rows * grid * floats.shape[1] * 8,
            bytes_accessed=planes * rows * grid * 4,
            transcendentals=0,
        ),
        name="interpolate",
    )(count, floats, cells, tile)


def turns(grid, wave, place, quarter):
    whole = np.mod(wave * place + (grid // 4) * quarter, grid)
    return np.cos(2.0 * np.pi * whole / grid).astype(np.float32)


def wave_tables(grid, slabs, columns, waves):
    kx = np.arange(slabs * waves).reshape(slabs, 1, waves)
    part = np.arange(2)
    x = np.arange(grid)
    table_x = turns(grid, kx[None], x[:, None, None, None], part[None, None, :, None])
    kz = np.arange(grid).reshape(columns, 1, grid // columns, 1, 1)
    table_z = turns(
        grid, kz, x[None, None, None, :, None],
        part[None, :, None, None, None] - part[None, None, None, None, :],
    ).reshape(2 * grid, 2 * grid)
    y = np.arange(grid).reshape(columns, 1, grid // columns, 1, 1)
    table_y = turns(
        grid, x[None, None, None, None, :], y,
        part[None, None, None, :, None] - part[None, :, None, None, None],
    )
    return table_x, table_z, table_y


def signed_wave(waves, grid):
    return jnp.where(waves < grid // 2, waves, waves - grid)


def influence(moduli, screening, slab, column, grid, count_kx, count_kz):
    kx = slab * count_kx + lax.iota(jnp.int32, count_kx)
    kz = column * count_kz + lax.iota(jnp.int32, count_kz)
    ky = lax.iota(jnp.int32, grid)
    half = grid // 2
    share = jnp.where((kx == 0) | (kx == half), 1.0, 2.0)
    share = jnp.where(kx <= half, share, 0.0) * (0.5 * coulomb / grid**3)
    nx, nz, ny = (signed_wave(k, grid) for k in (kx, kz, ky))
    radius = (nz * nz)[:, None, None] + (nx * nx)[None, :, None] + (ny * ny)[None, None, :]
    squared = radius.astype(jnp.float32) / float(grid * grid)
    mirrored = jnp.roll(moduli[:, ::-1], 1, 1)
    spare = jnp.zeros((count_kx * lax.axis_size("gz"),), jnp.float32)

    def product(table):
        mx = lax.dynamic_slice_in_dim(
            jnp.concatenate([table[2], spare]), slab * count_kx, count_kx, 0
        )
        mz = lax.dynamic_slice_in_dim(table[0], column * count_kz, count_kz, 0)
        return mz[:, None, None] * (share * mx)[None, :, None] * table[1][None, None, :]

    both = product(moduli) + product(mirrored)
    safe = jnp.where(radius > 0, squared, 1.0)
    return jnp.where(radius > 0, both * jnp.exp(-screening[0] * squared) / safe, 0.0)


def exchange(x, axis):
    return lax.all_to_all(x, axis, split_axis=0, concat_axis=0, tiled=True)


def contract(form, *operands):
    return jnp.einsum(form, *operands, precision=high, preferred_element_type=jnp.float32)


def potential_field(block, kernel, tables, slabs, columns, waves):
    table_x, table_z, table_y = tables
    planes, rows, grid = block.shape
    lanes = waves * rows
    spectrum = contract("zyx,xpck->pzcky", block, table_x)
    spectrum = exchange(spectrum.reshape(slabs * planes * 2, lanes), "gz")
    spectrum = contract("mn,nl->ml", table_z, spectrum)
    spectrum = exchange(spectrum, "gy").reshape(columns, 2, grid // columns, waves, rows)
    spectrum = contract("pczky,pcydw->zkdw", spectrum, table_y)
    spectrum = spectrum * kernel[:, :, None, :]
    spectrum = contract("zkdw,pcydw->pczky", spectrum, table_y)
    spectrum = exchange(spectrum.reshape(2 * grid, lanes), "gy")
    spectrum = contract("mn,ml->nl", table_z, spectrum)
    spectrum = exchange(spectrum, "gz").reshape(slabs, planes, 2, waves, rows)
    return contract("pzcky,xpck->zyx", spectrum, table_x)


def solve_tile(volume, kernel, tables, planes, rows, waves, slabs, columns):
    span_planes, span_rows, grid = volume.shape
    rim_planes = shifted(volume[planes : planes + 3], "gz", 1)
    volume = jnp.concatenate([volume[:3] + rim_planes, volume[3:planes]], 0)
    rim_rows = shifted(volume[:, rows : rows + 3], "gy", 1)
    block = jnp.concatenate([volume[:, :3] + rim_rows, volume[:, 3:rows]], 1)
    potential = potential_field(block, kernel, tables, slabs, columns, waves)
    upper_rows = shifted(potential[:, :3], "gy", -1)
    spare_rows = jnp.zeros((planes, span_rows - rows - 3, grid), jnp.float32)
    widened = jnp.concatenate([potential, upper_rows, spare_rows], 1)
    upper_planes = shifted(widened[:3], "gz", -1)
    spare_planes = jnp.zeros((span_planes - planes - 3, span_rows, grid), jnp.float32)
    return jnp.concatenate([widened, upper_planes, spare_planes], 0)


def body(charge, fractions, cell_base, live_blocks, send_blocks, moduli, screening):
    slabs = lax.axis_size("gz")
    columns = lax.axis_size("gy")
    grid = moduli.shape[1]
    planes = grid // slabs
    rows = grid // columns
    span_planes = round_up(planes + 3, 2)
    span_rows = round_up(rows + 3, 8)
    waves = -(-(grid // 2 + 1) // slabs)
    slab = lax.axis_index("gz")
    column = lax.axis_index("gy")
    lane_ids = lax.iota(jnp.int32, columns)
    live = jnp.sum(jnp.where(lane_ids == column, live_blocks[0], 0))
    send = jnp.sum(jnp.where(lane_ids == column, send_blocks[0], 0))
    before = jnp.sum(
        jnp.where(lane_ids == jnp.mod(column - 1, columns), send_blocks[0], 0)
    )
    kept_atoms = (live - send) * BLOCK
    moved_count = (before * BLOCK)[None]
    margin = SEND_MAX * BLOCK
    own_floats = jnp.concatenate([charge[None, :], fractions], 0)
    float_rows = jnp.concatenate([own_floats, jnp.zeros((4, margin), jnp.float32)], 1)
    cell_rows = jnp.concatenate([cell_base, jnp.zeros((3, margin), jnp.int32)], 1)
    lent_floats = lax.dynamic_slice_in_dim(float_rows, kept_atoms, margin, 1)
    lent_cells = lax.dynamic_slice_in_dim(cell_rows, kept_atoms, margin, 1)
    moved = shifted(lent_floats, "gy", 1)
    moved_cells = shifted(lent_cells, "gy", 1)
    sizes = (span_planes, span_rows, grid)
    tables = wave_tables(grid, slabs, columns, waves)
    kernel = influence(moduli, screening, slab, column, grid, waves, grid // columns)
    foreign = spread_atoms(moved_count, moved, moved_cells, *sizes)
    own_count, foreign, kernel = lax.optimization_barrier((kept_atoms[None], foreign, kernel))
    returned = shifted(foreign, "gy", -1)
    own = spread_atoms(own_count, own_floats, cell_base, *sizes)
    padded = solve_tile(
        (own + returned).reshape(sizes), kernel, tables, planes, rows, waves, slabs, columns
    ).reshape(span_planes * span_rows, grid)
    borrowed = shifted(padded, "gy", 1)
    own_forces = interpolate_atoms(own_count, own_floats, cell_base, padded, *sizes)
    own_forces, borrowed = lax.optimization_barrier((own_forces, borrowed))
    arrivals = interpolate_atoms(moved_count, moved, moved_cells, borrowed, *sizes)
    holder = jnp.zeros((3, charge.shape[0] + margin), jnp.float32)
    holder = lax.dynamic_update_slice(holder, arrivals, (jnp.zeros((), jnp.int32), kept_atoms))
    return own_forces + holder[:, : charge.shape[0]]


def solution(mesh):
    return jax.shard_map(
        body,
        mesh=mesh,
        in_specs=(
            P(("gz", "gy")),
            P(None, ("gz", "gy")),
            P(None, ("gz", "gy")),
            P("gz", None),
            P("gz", None),
            P(),
            P(),
        ),
        out_specs=P(None, ("gz", "gy")),
        check_vma=False,
    )
```
